8 devices in a mesh: tp: 2 (over z, y), dp: 4 (over x, core).
Axes of the slice: x: 2, y: 2, z: 1, core: 2. Of those that a mesh axis runs over, the one named last changes fastest.
Arguments:
- x_in: bfloat16 [32, 512, 3840], P('dp')
- dy_in: bfloat16 [32, 512, 3840], P('dp')
- positions: int32 [32, 512], P('dp')
- g_attn: bfloat16 [3840], replicated
- q_gain: bfloat16 [256], replicated
- k_gain: bfloat16 [256], replicated
- w_q: bfloat16 [3840, 4096], P(None, 'tp')
- w_k: bfloat16 [3840, 2048], P(None, 'tp')
- w_v: bfloat16 [3840, 2048], P(None, 'tp')
- w_o: bfloat16 [4096, 3840], P('tp')
Outputs:
- output 1: bfloat16 [32, 512, 3840], P('dp')
- output 2: bfloat16 [32, 512, 3840], P('dp')
- output 3: float32 [3840, 4096], P(None, 'tp')
- output 4: float32 [3840, 2048], P(None, 'tp')
- output 5: float32 [3840, 2048], P(None, 'tp')
- output 6: float32 [4096, 3840], P('tp')
- output 7: float32 [256], replicated
- output 8: float32 [256], replicated
- output 9: float32 [3840], replicated
All inputs are finite; a program needn't handle non-finite values.
Results may differ from the reference program's by a relative error of at most 0.0184639.
Values sent between devices are 32-bit elements.
A program may use at most 1 GiB of HBM per device.

```python
import jax
import jax.numpy as jnp
from jax import lax

BATCH_ROWS = 32
SEQ_LEN = 512
MODEL_DIM = 3840
NUM_HEADS = 16
KV_HEADS = 8
HEAD_DIM = 256
EPS = 1e-6
ROPE_THETA = 1000000.0
GROUP_SIZE = NUM_HEADS // KV_HEADS
ATT_SCALE = HEAD_DIM ** -0.5


def setup_inputs(seed: int = 0) -> dict:
    rng_keys = jax.random.split(jax.random.key(seed), 10)
    tok_shape = (BATCH_ROWS, SEQ_LEN, MODEL_DIM)
    x_in = jax.random.normal(rng_keys[0], tok_shape, jnp.float32).astype(jnp.bfloat16)
    dy_in = jax.random.normal(rng_keys[1], tok_shape, jnp.float32).astype(jnp.bfloat16)
    pos_steps = jax.random.randint(rng_keys[2], (BATCH_ROWS, SEQ_LEN), 1, 4, dtype=jnp.int32)
    positions = (jnp.cumsum(pos_steps, axis=1) - pos_steps[:, :1]).astype(jnp.int32)
    g_attn = (1.0 + 0.4 * jax.random.normal(rng_keys[3], (MODEL_DIM,), jnp.float32)).astype(jnp.bfloat16)
    q_gain = (1.0 + 0.5 * jax.random.normal(rng_keys[4], (HEAD_DIM,), jnp.float32)).astype(jnp.bfloat16)
    k_gain = (1.0 + 0.5 * jax.random.normal(rng_keys[5], (HEAD_DIM,), jnp.float32)).astype(jnp.bfloat16)
    in_scale = MODEL_DIM ** -0.5
    w_q = (jax.random.normal(rng_keys[6], (MODEL_DIM, NUM_HEADS * HEAD_DIM), jnp.float32) * in_scale).astype(jnp.bfloat16)
    w_k = (jax.random.normal(rng_keys[7], (MODEL_DIM, KV_HEADS * HEAD_DIM), jnp.float32) * in_scale).astype(jnp.bfloat16)
    w_v = (jax.random.normal(rng_keys[8], (MODEL_DIM, KV_HEADS * HEAD_DIM), jnp.float32) * in_scale).astype(jnp.bfloat16)
    w_o = (jax.random.normal(rng_keys[9], (NUM_HEADS * HEAD_DIM, MODEL_DIM), jnp.float32) * (NUM_HEADS * HEAD_DIM) ** -0.5).astype(jnp.bfloat16)
    return {"x_in": x_in, "dy_in": dy_in, "positions": positions, "g_attn": g_attn, "q_gain": q_gain, "k_gain": k_gain, "w_q": w_q, "w_k": w_k, "w_v": w_v, "w_o": w_o}


def rope_tables(positions):
    inv_freq = ROPE_THETA ** (-jnp.arange(0, HEAD_DIM, 2, dtype=jnp.float32) / HEAD_DIM)
    angles = positions.astype(jnp.float32)[:, :, None, None] * inv_freq
    return jnp.cos(angles), jnp.sin(angles)


def head_norm_rope(t_proj, weight, cos_tab, sin_tab):
    t_f32 = t_proj.astype(jnp.float32)
    t_hat = t_f32 * lax.rsqrt(jnp.mean(t_f32 * t_f32, axis=-1, keepdims=True) + EPS)
    scaled = t_hat * weight
    half_dim = HEAD_DIM // 2
    low_half = scaled[..., :half_dim]
    high_half = scaled[..., half_dim:]
    return jnp.concatenate([low_half * cos_tab - high_half * sin_tab, high_half * cos_tab + low_half * sin_tab], axis=-1)


def attend_row(row_args):
    q_row, k_row, v_row, do_row = row_args
    q_grp = q_row.reshape(SEQ_LEN, KV_HEADS, GROUP_SIZE, HEAD_DIM).astype(jnp.float32)
    do_grp = do_row.reshape(SEQ_LEN, KV_HEADS, GROUP_SIZE, HEAD_DIM).astype(jnp.float32)
    k_f32 = k_row.astype(jnp.float32)
    v_f32 = v_row.astype(jnp.float32)
    scores = jnp.einsum("qkgd,skd->kgqs", q_grp, k_f32) * ATT_SCALE
    causal = jnp.arange(SEQ_LEN)[:, None] >= jnp.arange(SEQ_LEN)[None, :]
    attn_prob = jax.nn.softmax(jnp.where(causal, scores, -jnp.inf), axis=-1)
    prob_bf = attn_prob.astype(jnp.bfloat16).astype(jnp.float32)
    row_out = jnp.einsum("kgqs,skd->qkgd", prob_bf, v_f32).astype(jnp.bfloat16)
    d_val = jnp.einsum("kgqs,qkgd->skd", prob_bf, do_grp).astype(jnp.bfloat16)
    d_prob = jnp.einsum("qkgd,skd->kgqs", do_grp, v_f32)
    d_score = attn_prob * (d_prob - jnp.sum(d_prob * attn_prob, axis=-1, keepdims=True)) * ATT_SCALE
    ds_bf = d_score.astype(jnp.bfloat16).astype(jnp.float32)
    d_query = jnp.einsum("kgqs,skd->qkgd", ds_bf, k_f32).astype(jnp.bfloat16)
    d_key = jnp.einsum("kgqs,qkgd->skd", ds_bf, q_grp).astype(jnp.bfloat16)
    return (row_out.reshape(SEQ_LEN, NUM_HEADS, HEAD_DIM), d_query.reshape(SEQ_LEN, NUM_HEADS, HEAD_DIM), d_key, d_val)


def reference(x_in, dy_in, positions, g_attn, q_gain, k_gain, w_q, w_k, w_v, w_o):
    x_f32 = x_in.astype(jnp.float32).reshape(-1, MODEL_DIM)
    inv_rms = lax.rsqrt(jnp.mean(x_f32 * x_f32, axis=-1, keepdims=True) + EPS)
    x_hat = x_f32 * inv_rms
    normed = (x_hat * g_attn.astype(jnp.float32)).astype(jnp.bfloat16)
    q_raw = jnp.dot(normed, w_q, preferred_element_type=jnp.float32).astype(jnp.bfloat16).reshape(BATCH_ROWS, SEQ_LEN, NUM_HEADS, HEAD_DIM)
    k_raw = jnp.dot(normed, w_k, preferred_element_type=jnp.float32).astype(jnp.bfloat16).reshape(BATCH_ROWS, SEQ_LEN, KV_HEADS, HEAD_DIM)
    v_proj = jnp.dot(normed, w_v, preferred_element_type=jnp.float32).astype(jnp.bfloat16).reshape(BATCH_ROWS, SEQ_LEN, KV_HEADS, HEAD_DIM)
    cos_tab, sin_tab = rope_tables(positions)
    q_rot, q_pull = jax.vjp(lambda t_proj, weight: head_norm_rope(t_proj, weight, cos_tab, sin_tab), q_raw, q_gain.astype(jnp.float32))
    k_rot, k_pull = jax.vjp(lambda t_proj, weight: head_norm_rope(t_proj, weight, cos_tab, sin_tab), k_raw, k_gain.astype(jnp.float32))
    dy_flat = dy_in.reshape(-1, MODEL_DIM)
    d_out = jnp.dot(dy_flat, w_o.T, preferred_element_type=jnp.float32).astype(jnp.bfloat16).reshape(BATCH_ROWS, SEQ_LEN, NUM_HEADS, HEAD_DIM)
    attn_out, dq_rot, dk_rot, dv_proj = lax.map(attend_row, (q_rot.astype(jnp.bfloat16), k_rot.astype(jnp.bfloat16), v_proj, d_out))
    o_flat = attn_out.reshape(-1, NUM_HEADS * HEAD_DIM)
    attn_sum = jnp.dot(o_flat, w_o, preferred_element_type=jnp.float32)
    y_out = (x_f32 + attn_sum).astype(jnp.bfloat16).reshape(x_in.shape)
    dw_o = jnp.dot(o_flat.T, dy_flat, preferred_element_type=jnp.float32)
    dq_raw, dq_gain = q_pull(dq_rot.astype(jnp.float32))
    dk_raw, dk_gain = k_pull(dk_rot.astype(jnp.float32))
    dq_flat = dq_raw.reshape(-1, NUM_HEADS * HEAD_DIM)
    dk_flat = dk_raw.reshape(-1, KV_HEADS * HEAD_DIM)
    dv_flat = dv_proj.reshape(-1, KV_HEADS * HEAD_DIM)
    dw_q = jnp.dot(normed.T, dq_flat, preferred_element_type=jnp.float32)
    dw_k = jnp.dot(normed.T, dk_flat, preferred_element_type=jnp.float32)
    dw_v = jnp.dot(normed.T, dv_flat, preferred_element_type=jnp.float32)
    d_normed = (jnp.dot(dq_flat, w_q.T, preferred_element_type=jnp.float32) + jnp.dot(dk_flat, w_k.T, preferred_element_type=jnp.float32) + jnp.dot(dv_flat, w_v.T, preferred_element_type=jnp.float32))
    dg_attn = jnp.sum(d_normed * x_hat, axis=0)
    d_scaled = d_normed * g_attn.astype(jnp.float32)
    dx_f32 = dy_flat.astype(jnp.float32) + inv_rms * (d_scaled - x_hat * jnp.mean(d_scaled * x_hat, axis=-1, keepdims=True))
    dx_out = dx_f32.astype(jnp.bfloat16).reshape(x_in.shape)
    return (y_out, dx_out, dw_q, dw_k, dw_v, dw_o, dq_gain, dk_gain, dg_attn)
```

```python
import functools

import jax
import jax.numpy as jnp
from jax import lax
from jax.experimental import pallas as pl
from jax.experimental.pallas import tpu as pltpu
from jax.sharding import PartitionSpec as P


EPS = 1e-6
ROPE_THETA = 1000000.0
LOG2_E = 1.4426950408889634
Q_BLOCK = 256

SWAP_TP = [(0, 1), (1, 0)]


def head_norm(t_raw, eps_dim):
    t_f32 = t_raw.astype(jnp.float32)
    inv = lax.rsqrt(jnp.sum(t_f32 * t_f32, axis=-1, keepdims=True) * (1.0 / eps_dim) + EPS)
    return t_f32 * inv, inv


def rope(u, cos, sin):
    half = u.shape[-1] // 2
    low, high = u[:, :half], u[:, half:]
    return jnp.concatenate([low * cos - high * sin, high * cos + low * sin], axis=-1)


def unrope(g, cos, sin):
    half = g.shape[-1] // 2
    low, high = g[:, :half], g[:, half:]
    return jnp.concatenate([low * cos + high * sin, high * cos - low * sin], axis=-1)


def norm_pull(d_rot, t_hat, inv, gain, cos, sin):
    d_u = unrope(d_rot.astype(jnp.float32), cos, sin)
    by_gain = d_u * t_hat
    d_gain = jnp.sum(by_gain.reshape(-1, 8, by_gain.shape[-1]), axis=0)
    d_hat = d_u * gain
    mean = jnp.sum(d_hat * t_hat, axis=-1, keepdims=True) * (1.0 / t_hat.shape[-1])
    return (inv * (d_hat - t_hat * mean)).astype(jnp.bfloat16), d_gain


def attend(group, dim, qkv_ref, do_ref, cos_ref, sin_ref, qg_ref, kg_ref, o_ref, d_ref, gq_ref, gk_ref, dv_acc, dk_acc):
    seq = qkv_ref.shape[0]
    scale = dim ** -0.5
    cos, sin = cos_ref[...], sin_ref[...]
    q_gain, k_gain = qg_ref[...], kg_ref[...]
    k_hat, k_inv = head_norm(qkv_ref[:, group * dim:(group + 1) * dim], dim)
    k_rot = rope(k_hat * k_gain, cos, sin).astype(jnp.bfloat16)
    v = qkv_ref[:, (group + 1) * dim:]
    nt = (((1,), (1,)), ((), ()))
    tn = (((0,), (0,)), ((), ()))
    dot = functools.partial(lax.dot_general, preferred_element_type=jnp.float32)
    d_gain_q = jnp.zeros((8, dim), jnp.float32)
    dv_acc[...] = jnp.zeros_like(dv_acc)
    dk_acc[...] = jnp.zeros_like(dk_acc)
    for head in range(group):
        cols = slice(head * dim, (head + 1) * dim)
        q_hat, q_inv = head_norm(qkv_ref[:, cols], dim)
        q_rot = rope(q_hat * q_gain, cos, sin).astype(jnp.bfloat16)
        d_out = do_ref[:, cols]
        parts = []
        for start in range(0, seq, Q_BLOCK):
            stop = start + Q_BLOCK
            q_blk, do_blk = q_rot[start:stop], d_out[start:stop]
            s = dot(k_rot[:stop], q_blk, nt)
            key = lax.broadcasted_iota(jnp.int32, s.shape, 0)
            query = lax.broadcasted_iota(jnp.int32, s.shape, 1) + start
            s = jnp.where(key <= query, s, -jnp.inf)
            e = jnp.exp2((s - jnp.max(s, axis=0, keepdims=True)) * (scale * LOG2_E))
            prob = e * (1.0 / jnp.sum(e, axis=0, keepdims=True))
            prob_bf = prob.astype(jnp.bfloat16)
            d_prob = dot(v[:stop], do_blk, nt)
            row = jnp.sum(prob * d_prob, axis=0, keepdims=True)
            d_score = (prob * (d_prob - row) * scale).astype(jnp.bfloat16)
            o_ref[start:stop, cols] = dot(prob_bf, v[:stop], tn).astype(jnp.bfloat16)
            parts.append(dot(d_score, k_rot[:stop], tn).astype(jnp.bfloat16))
            dv_acc[:stop] += lax.dot(prob_bf, do_blk, preferred_element_type=jnp.float32)
            dk_acc[:stop] += lax.dot(d_score, q_blk, preferred_element_type=jnp.float32)
        d_raw, d_gain = norm_pull(jnp.concatenate(parts, axis=0), q_hat, q_inv, q_gain, cos, sin)
        d_ref[:, cols] = d_raw
        d_gain_q += d_gain
    dk_raw, d_gain_k = norm_pull(dk_acc[...].astype(jnp.bfloat16), k_hat, k_inv, k_gain, cos, sin)
    d_ref[:, group * dim:(group + 1) * dim] = dk_raw
    d_ref[:, (group + 1) * dim:] = dv_acc[...].astype(jnp.bfloat16)
    gq_ref[...] = d_gain_q
    gk_ref[...] = d_gain_k


def attention(qkv, d_out, cos, sin, q_gain, k_gain, seq, group, dim):
    rows = qkv.shape[0] // seq
    width = (group + 2) * dim
    kv = qkv.shape[1] // width
    by_head = lambda b, h: (b, h)
    by_row = lambda b, h: (b, 0)
    whole = lambda b, h: (0, 0)
    steps = rows * kv
    flops = 6 * 2 * steps * group * seq * seq * dim * 3 // 4
    return pl.pallas_call(
        functools.partial(attend, group, dim),
        grid=(rows, kv),
        in_specs=[
            pl.BlockSpec((seq, width), by_head),
            pl.BlockSpec((seq, group * dim), by_head),
            pl.BlockSpec((seq, dim // 2), by_row),
            pl.BlockSpec((seq, dim // 2), by_row),
            pl.BlockSpec((1, dim), whole),
            pl.BlockSpec((1, dim), whole),
        ],
        out_specs=[
            pl.BlockSpec((seq, group * dim), by_head),
            pl.BlockSpec((seq, width), by_head),
            pl.BlockSpec((8, dim), by_head),
            pl.BlockSpec((8, dim), by_head),
        ],
        out_shape=[
            jax.ShapeDtypeStruct(d_out.shape, jnp.bfloat16),
            jax.ShapeDtypeStruct(qkv.shape, jnp.bfloat16),
            jax.ShapeDtypeStruct((rows * 8, kv * dim), jnp.float32),
            jax.ShapeDtypeStruct((rows * 8, kv * dim), jnp.float32),
        ],
        scratch_shapes=[pltpu.VMEM((seq, dim), jnp.float32), pltpu.VMEM((seq, dim), jnp.float32)],
        compiler_params=pltpu.CompilerParams(dimension_semantics=("arbitrary", "arbitrary"), vmem_limit_bytes=48 * 1024 * 1024),
        cost_estimate=pl.CostEstimate(flops=flops, bytes_accessed=2 * (qkv.size + d_out.size) * 2, transcendentals=steps * group * seq * seq),
        name="attend",
    )(qkv, d_out, cos, sin, q_gain, k_gain)


def interleave(w_q, w_k, w_v, groups, group, dim):
    cols = []
    for g in groups:
        cols += [w_q[:, g * group * dim:(g + 1) * group * dim], w_k[:, g * dim:(g + 1) * dim], w_v[:, g * dim:(g + 1) * dim]]
    return jnp.concatenate(cols, axis=1)


def dot_nn(a, b):
    return jnp.dot(a, b, preferred_element_type=jnp.float32)


def dot_nt(a, b):
    return jnp.einsum("td,id->ti", a, b, preferred_element_type=jnp.float32)


def dot_tn(a, b):
    return jnp.einsum("td,ti->di", a, b, preferred_element_type=jnp.float32)


def fetch_half(w, core):
    half = w.shape[0] // 2
    send = lax.dynamic_slice_in_dim(w, core * half, half, 0).astype(jnp.float32)
    return lax.ppermute(send, "tp", SWAP_TP)


def join_body(core_ref, near_ref, far_ref, full_ref):
    mine = pl.program_id(0) == core_ref[0]

    @pl.when(mine)
    def _():
        full_ref[...] = near_ref[...].astype(full_ref.dtype)

    @pl.when(jnp.logical_not(mine))
    def _():
        full_ref[...] = far_ref[...].astype(full_ref.dtype)


JOIN_ROWS = 128


def join_halves(near, core, core_swap):
    far = lax.ppermute(near, "dp", core_swap)
    half, width = near.shape
    blocks = half // JOIN_ROWS
    return pl.pallas_call(
        join_body,
        grid_spec=pltpu.PrefetchScalarGridSpec(
            num_scalar_prefetch=1,
            grid=(2, blocks),
            in_specs=[
                pl.BlockSpec((JOIN_ROWS, width), lambda h, i, c: (jnp.where(h == c[0], i, 0), 0)),
                pl.BlockSpec((JOIN_ROWS, width), lambda h, i, c: (jnp.where(h == c[0], 0, i), 0)),
            ],
            out_specs=pl.BlockSpec((JOIN_ROWS, width), lambda h, i, c: (h * blocks + i, 0)),
        ),
        out_shape=jax.ShapeDtypeStruct((2 * half, width), jnp.bfloat16),
        compiler_params=pltpu.CompilerParams(dimension_semantics=("arbitrary", "arbitrary")),
        cost_estimate=pl.CostEstimate(flops=2 * half * width * 32, bytes_accessed=12 * half * width, transcendentals=0),
        name="join",
    )(core.reshape(1), near, far)


CHUNKS = 2


def solution(mesh):
    tok_spec = P("dp", None, None)
    col_spec = P(None, "tp")
    row_spec = P("tp", None)
    n_dp = mesh.shape["dp"]
    core_swap = [(i, i ^ 1) for i in range(n_dp)]
    chip_swap = [(i, (i + 2) % n_dp) for i in range(n_dp)]
    cores = [[i, i + 1] for i in range(0, n_dp, 2)]

    def per_device(x_in, dy_in, positions, g_attn, q_gain, k_gain, w_q, w_k, w_v, w_o):
        _, n_seq, n_dim = x_in.shape
        dim = q_gain.shape[0]
        n_kv = w_k.shape[1] // dim
        group = w_q.shape[1] // w_k.shape[1]
        core = lax.rem(lax.axis_index("dp"), 2)
        chip = lax.div(lax.axis_index("dp"), 2)
        tp = lax.axis_index("tp")
        size = n_kv // CHUNKS
        own = []
        for c in range(CHUNKS):
            w_cat = interleave(w_q, w_k, w_v, range(c * size, (c + 1) * size), group, dim)
            own.append((w_cat, w_o[c * size * group * dim:(c + 1) * size * group * dim]))
        near = [(fetch_half(w_cat, core), fetch_half(w_out, core)) for w_cat, w_out in own]

        x_f32 = x_in.astype(jnp.float32).reshape(-1, n_dim)
        inv_rms = lax.rsqrt(jnp.mean(x_f32 * x_f32, axis=-1, keepdims=True) + EPS)
        x_hat = x_f32 * inv_rms
        normed = (x_hat * g_attn.astype(jnp.float32)).astype(jnp.bfloat16)
        dy_flat = dy_in.reshape(-1, n_dim)
        inv_freq = ROPE_THETA ** (-jnp.arange(0, dim, 2, dtype=jnp.float32) / dim)
        angles = positions.astype(jnp.float32).reshape(-1, 1) * inv_freq
        cos, sin = jnp.cos(angles), jnp.sin(angles)
        q_gain_f32 = q_gain.astype(jnp.float32).reshape(1, dim)
        k_gain_f32 = k_gain.astype(jnp.float32).reshape(1, dim)

        def heads(w_cat, w_out):
            qkv = dot_nn(normed, w_cat).astype(jnp.bfloat16)
            d_out = dot_nt(dy_flat, w_out).astype(jnp.bfloat16)
            return attention(qkv, d_out, cos, sin, q_gain_f32, k_gain_f32, n_seq, group, dim)

        def reduce_dp(part):
            part = lax.psum_scatter(part, "dp", scatter_dimension=0, axis_index_groups=cores, tiled=True)
            half = part.shape[0] // 2
            keep = lax.dynamic_slice_in_dim(part, chip * half, half, 0)
            send = lax.dynamic_slice_in_dim(part, (1 - chip) * half, half, 0)
            got = lax.ppermute(send, "dp", chip_swap)
            keep = keep + got
            got = lax.ppermute(keep, "dp", chip_swap)
            part = lax.dynamic_update_slice_in_dim(part, keep, chip * half, 0)
            part = lax.dynamic_update_slice_in_dim(part, got, (1 - chip) * half, 0)
            return lax.all_gather(part, "dp", axis_index_groups=cores, axis=0, tiled=True)

        def sums(o, d, w_cat, w_out, a_sum, d_sum):
            a_part = dot_nn(o, w_out)
            a_sum = a_part if a_sum is None else a_sum + a_part
            d_part = dot_nt(d, w_cat)
            d_sum = d_part if d_sum is None else d_sum + d_part
            return a_sum, d_sum

        dw_cat, dw_out, gq, gk = [], [], 0.0, 0.0
        a_own = d_own = a_far = d_far = None
        for w_cat, w_out in own:
            o, d, gq_part, gk_part = heads(w_cat, w_out)
            gq += jnp.sum(gq_part.reshape(-1, size, dim), axis=(0, 1))
            gk += jnp.sum(gk_part.reshape(-1, size, dim), axis=(0, 1))
            dw = dot_tn(normed, d)
            dw_cat.append(reduce_dp(dw))
            dw = dot_tn(o, dy_flat)
            dw_out.append(reduce_dp(dw))
            a_own, d_own = sums(o, d, w_cat, w_out, a_own, d_own)
        for c, (w_near, o_near) in enumerate(near):
            w_cat = join_halves(w_near, core, core_swap)
            w_out = join_halves(o_near, core, core_swap)
            o, d, _, _ = heads(w_cat, w_out)
            a_far, d_far = sums(o, d, w_cat, w_out, a_far, d_far)
            if c + 1 < CHUNKS:
                a_far, d_far = lax.optimization_barrier((a_far, d_far))

        y_out = (x_f32 + (a_own + a_far)).astype(jnp.bfloat16).reshape(x_in.shape)
        d_sum = d_own + d_far
        d_scaled = d_sum * g_attn.astype(jnp.float32)
        dx_f32 = dy_flat.astype(jnp.float32) + inv_rms * (d_scaled - x_hat * jnp.mean(d_scaled * x_hat, axis=-1, keepdims=True))
        dx_out = dx_f32.astype(jnp.bfloat16).reshape(x_in.shape)
        dg_part = jnp.sum(d_sum * x_hat, axis=0)
        mine = (jnp.arange(n_dim) < n_dim // 2) == (tp == 0)
        dg_part = jnp.where(mine, dg_part, 0.0)
        small = lax.psum(jnp.concatenate([gq, gk, dg_part]), ("tp", "dp"))

        wide = (group + 2) * dim

        def columns(start, stop):
            return jnp.concatenate([t[:, h * wide + start * dim:h * wide + stop * dim] for t in dw_cat for h in range(size)], axis=1)

        dw_q, dw_k, dw_v = columns(0, group), columns(group, group + 1), columns(group + 1, group + 2)
        dw_o = jnp.concatenate(dw_out, axis=0)
        return y_out, dx_out, dw_q, dw_k, dw_v, dw_o, small[:dim], small[dim:2 * dim], small[2 * dim:]

    return jax.shard_map(per_device, mesh=mesh, in_specs=(tok_spec, tok_spec, P("dp", None), P(), P(), P(), col_spec, col_spec, col_spec, row_spec), out_specs=(tok_spec, tok_spec, col_spec, col_spec, col_spec, row_spec, P(), P(), P()), check_vma=False)
```
